32 devices in a mesh: layer: 2 (over core), row: 16 (over z, y, x).
Axes of the slice: x: 2, y: 2, z: 4, core: 2. Of those that a mesh axis runs over, the one named last changes fastest.
Arguments:
- sources: bfloat16 [2, 4608, 512], P('layer', 'row'), may hold values from -2 to 2
- green_down: bfloat16 [2, 4608, 4608], P('layer', 'row')
- green_up: bfloat16 [2, 4608, 4608], P('layer', 'row')
- material: int32 [8, 4608], P('layer', 'row'), may hold values 0 or 1
- pml_cells: int32 [1], replicated, may hold values from 4 to 39
Outputs:
- residual: bfloat16 [8, 4608, 512], P('layer', 'row')
The draws below stay inside these ranges and needn't reach their ends.
All inputs are finite; a program needn't handle non-finite values. No bound on the sum of `material` on one device may be relied on, other than what follows from the above.
Results may differ from the reference program's by a relative error of at most 0.005.
Values may be sent and summed in bfloat16 or wider, within the bound.
No kernel may reach another device: no remote copies, remote signals or barrier semaphores. Data moves between devices by JAX's collectives and lax.ppermute only.
A program may use at most 64 MiB of HBM per device.

```python
import jax
import jax.numpy as jnp
from jax import lax

M = 4608
K = 4
LAYERS = 2
SRC = 512
ZS = 8


def green_matrix(key):
    key_diag, key_rest = jax.random.split(key)
    diag = jax.random.uniform(key_diag, (LAYERS, 1, 1), jnp.float32, 0.8, 0.93)
    rest = jax.random.normal(key_rest, (LAYERS, M, M), jnp.float32)
    eye = jnp.eye(M, dtype=jnp.float32)[None]
    return (diag * eye + 0.3 * rest / jnp.sqrt(float(M))).astype(jnp.bfloat16)


def draw_green_down(key, part):
    return green_matrix(jax.random.fold_in(key, 11))


def draw_green_up(key, part):
    return green_matrix(jax.random.fold_in(key, 23))


def plant(values, rng, least, high):
    shape = values.shape
    spot = [jax.random.randint(jax.random.fold_in(rng, axis), (), 0, shape[axis]) for axis in range(len(shape))]
    values = values.at[tuple(spot)].set(least)
    longest = shape.index(max(shape))
    spot[longest] = (spot[longest] + 1) % shape[longest]
    return values.at[tuple(spot)].set(high)


def steps_of(rng, shape, shards, least, largest):
    def one(axis_at, blocks):
        heights = jax.random.uniform(jax.random.fold_in(jax.random.fold_in(rng, 6), axis_at), (blocks,), jnp.float32, least / len(shards), largest / len(shards))
        return jnp.repeat(jnp.exp(heights), shape[axis_at] // blocks).reshape((-1,) + (1,) * (len(shape) - axis_at - 1))

    loudness = one(*shards[0])
    for cut in shards[1:]:
        loudness = loudness * one(*cut)
    return loudness


def noise(stream_key, extent, deviation, limit, cuts=(), kind=jnp.bfloat16):
    entries = jax.random.normal(stream_key, extent, jnp.float32) * deviation
    if len(cuts) > 0:
        entries = steps_of(stream_key, extent, cuts, -0.22, 0.18) * entries
    return jnp.clip(entries, min=-limit, max=limit).astype(kind)


def setup_inputs(seed: int = 0) -> dict:
    arg_keys = jax.random.split(jax.random.key(seed), 6)
    return {
        "sources": noise(arg_keys[0], (LAYERS, M, SRC), 0.3, 2.0, ((0, 2), (1, 16))),
        "green_down": draw_green_down(jax.random.fold_in(arg_keys[5], 71), 0),
        "green_up": draw_green_up(jax.random.fold_in(arg_keys[5], 71), 0),
        "material": plant((jax.random.randint(arg_keys[3], (ZS, M), 0, 2) < 1).astype(jnp.int32), jax.random.fold_in(arg_keys[3], 1), 0, 1),
        "pml_cells": jax.random.randint(arg_keys[4], (1,), 4, 40).astype(jnp.int32),
    }


def sweep(green, sources, reverse):
    def advance(carry, item):
        matrix, source = item
        entry = (source.astype(jnp.float32) + carry.astype(jnp.float32)).astype(jnp.bfloat16)
        result = jnp.dot(matrix.astype(jnp.float32), entry.astype(jnp.float32), precision=lax.Precision.HIGHEST).astype(jnp.bfloat16)
        return result, result
    start = jnp.zeros((M, SRC), jnp.bfloat16)
    unused, traces = lax.scan(advance, start, (green, sources), reverse=reverse)
    return traces


def ramp(index, count, thick):
    dist = jnp.minimum(index, count - 1 - index).astype(jnp.float32)
    return jnp.maximum(thick - dist, 0.0) / thick


def reference(sources, green_down, green_up, material, pml_cells):
    down = sweep(green_down, sources, False)
    up = sweep(green_up, sources, True)
    wave = sources.astype(jnp.float32) + down.astype(jnp.float32) + up.astype(jnp.float32)
    factor = (K - jnp.arange(K, dtype=jnp.float32)) / K
    slab = (wave[:, None, :, :] * factor[None, :, None, None]).reshape(ZS, M, SRC)
    thick = pml_cells[0].astype(jnp.float32)
    ramp_z = ramp(jnp.arange(ZS, dtype=jnp.int32), ZS, thick)
    ramp_m = ramp(jnp.arange(M, dtype=jnp.int32), M, thick)
    sigma = 3.0 * (ramp_z[:, None] * ramp_z[:, None] + ramp_m[None, :] * ramp_m[None, :])
    kappa = 1.0 + 1.5 * material.astype(jnp.float32)
    padded = jnp.pad(slab, ((1, 1), (1, 1), (0, 0)))
    beside = padded[2:, 1:-1] + padded[:-2, 1:-1] + padded[1:-1, 2:] + padded[1:-1, :-2]
    result = kappa[:, :, None] * ((4.0 + sigma)[:, :, None] * slab - beside)
    return result.astype(jnp.bfloat16)
```

```python
import jax
import jax.numpy as jnp
from jax import lax
from jax.sharding import PartitionSpec as P


def shifted(value, axis, steps):
    count = lax.axis_size(axis)
    leading, last = (max(0, -steps), min(count, count - steps))
    return lax.ppermute(value, axis, [(source, source + steps) for source in range(leading, last)])


def ramp(index, count, thick):
    dist = jnp.minimum(index, count - 1 - index).astype(jnp.float32)
    return jnp.maximum(thick - dist, 0.0) / thick


def gather(block):
    return lax.all_gather(block, "row", axis=0, tiled=True)


def residual_of(source, first, second, material, pml_cells, here, layers):
    rows, total = source.shape
    planes = material.shape[0]
    wave = source.astype(jnp.float32) + first.astype(jnp.float32) + second.astype(jnp.float32)
    factor = (planes - jnp.arange(planes, dtype=jnp.float32)) / planes
    sent = wave.astype(jnp.bfloat16)
    other = sent[None]
    before_plane = shifted(other, "layer", 1).astype(jnp.float32) * factor[planes - 1]
    after_plane = shifted(other, "layer", -1).astype(jnp.float32) * factor[0]
    before_row = shifted(sent[rows - 1 :], "row", 1).astype(jnp.float32)
    after_row = shifted(sent[:1], "row", -1).astype(jnp.float32)
    thick = pml_cells[0].astype(jnp.float32)
    plane_index = here * planes + jnp.arange(planes, dtype=jnp.int32)
    point_index = lax.axis_index("row") * rows + jnp.arange(rows, dtype=jnp.int32)
    ramp_z = ramp(plane_index, layers * planes, thick)
    ramp_m = ramp(point_index, rows * lax.axis_size("row"), thick)
    sigma = 3.0 * (ramp_z[:, None] * ramp_z[:, None] + ramp_m[None, :] * ramp_m[None, :])
    kappa = 1.0 + 1.5 * material.astype(jnp.float32)
    slab = wave[None] * factor[:, None, None]
    tall = jnp.concatenate([before_plane, slab, after_plane], axis=0)
    wide = jnp.concatenate([before_row, wave, after_row], axis=0)
    beside_rows = (wide[2:] + wide[:-2])[None] * factor[:, None, None]
    beside = tall[2:] + tall[:-2] + beside_rows
    result = kappa[:, :, None] * ((4.0 + sigma)[:, :, None] * slab - beside)
    return result.astype(jnp.bfloat16)


def local(sources, green_down, green_up, material, pml_cells):
    source = sources[0]
    layers = lax.axis_size("layer")
    here = lax.axis_index("layer")

    def multiply(pick_down, block):
        def with_matrix(matrix):
            return lambda: jnp.dot(matrix[0], block, preferred_element_type=jnp.float32)

        return lax.cond(pick_down, with_matrix(green_down), with_matrix(green_up)).astype(jnp.bfloat16)

    first = multiply(here == 0, gather(source))
    moved = lax.ppermute(first, "layer", [(0, 1), (1, 0)])
    entry = (source.astype(jnp.float32) + moved.astype(jnp.float32)).astype(jnp.bfloat16)
    second = multiply(here != 0, gather(entry))
    return residual_of(source, first, second, material, pml_cells, here, layers)


def solution(mesh):
    return jax.shard_map(
        local,
        mesh=mesh,
        in_specs=(
            P("layer", "row", None),
            P("layer", "row", None),
            P("layer", "row", None),
            P("layer", "row"),
            P(),
        ),
        out_specs=P("layer", "row", None),
        check_vma=False,
    )
```
